32 devices in a mesh: ta: 2 (over x), gx: 16 (over z, y, core).
Axes of the slice: x: 2, y: 2, z: 4, core: 2. Of those that a mesh axis runs over, the one named last changes fastest.
Arguments:
- voltages: bfloat16 [2, 128, 2, 256, 512], P('ta', 'gx'), may hold values from -6 to 6
- weights: bfloat16 [2, 256, 2, 512, 64], P(None, 'gx'), may hold values from -0.125 to 0.125
Outputs:
- spectra: float32 [256, 2, 512, 64], P(None, None, 'gx', 'ta')
The draws below stay inside these ranges and needn't reach their ends.
All inputs are finite; a program needn't handle non-finite values.
Results may differ from the reference program's by a relative error of at most 0.0003.
Values may be sent and summed in bfloat16 or wider, within the bound.
No kernel may reach another device: no remote copies, remote signals or barrier semaphores. Data moves between devices by JAX's collectives and lax.ppermute only.
A program may use at most 64 MiB of HBM per device.

```python
import jax
import jax.numpy as jnp
from jax import lax

ANTENNA_COUNT = 64
BEAM_TOTAL = 512
CHANNEL_COUNT = 512
HALF_SAMPLES = 512


def block_levels(own_key, shape, cuts, low, largest):
    factor_of = 1.0
    for position, blocks in cuts:
        draws = jax.random.uniform(jax.random.fold_in(jax.random.fold_in(own_key, 6), position), (blocks,), jnp.float32, low / len(cuts), largest / len(cuts))
        factor_of = factor_of * jnp.repeat(jnp.exp(draws), shape[position] // blocks).reshape((-1,) + (1,) * (len(shape) - 1 - position))
    return factor_of


def normal_values(rng, dims, scale, most, pieces=(), dtype=jnp.bfloat16):
    array = scale * jax.random.normal(rng, dims, jnp.float32)
    if pieces:
        array = array * block_levels(rng, dims, pieces, -0.22, 0.18)
    return jnp.clip(array, -most, most).astype(dtype)


def setup_inputs(seed: int = 0) -> dict:
    streams_of = jax.random.split(jax.random.key(seed), 3)
    voltages = normal_values(streams_of[0], (2, 2 * ANTENNA_COUNT, 2, CHANNEL_COUNT // 2, HALF_SAMPLES), 1.0, 6.0, ((0, 2), (1, 16)))
    weights = normal_values(streams_of[1], (2, CHANNEL_COUNT // 2, 2, BEAM_TOTAL, ANTENNA_COUNT), (32 * ANTENNA_COUNT) ** -0.5, 0.125, ((1, 16),))
    return dict(voltages=voltages, weights=weights)


def beam_power(voltage, weight_block):
    antennas = weight_block.shape[3]
    beam_count = weight_block.shape[2]
    powers = []
    for side_index in range(2):
        real_w = weight_block[side_index, 0]
        imag_w = weight_block[side_index, 1]
        upper_rows = jnp.stack([real_w, -imag_w], axis=-1).reshape(beam_count, 2 * antennas)
        bottom_half_rows = jnp.stack([imag_w, real_w], axis=-1).reshape(beam_count, 2 * antennas)
        matrix = jnp.concatenate([upper_rows, bottom_half_rows], 0)
        signal = voltage[side_index * antennas:(side_index + 1) * antennas].reshape(2 * antennas, -1)
        beam_voltage_field = jnp.dot(matrix, signal, preferred_element_type=jnp.float32)
        power = beam_voltage_field[:beam_count] * beam_voltage_field[:beam_count] + beam_voltage_field[beam_count:] * beam_voltage_field[beam_count:]
        powers.append(power.reshape(beam_count, -1, 8).sum(-1))
    return jnp.stack(powers, 0)


def reference(voltages, weights):
    moved = jnp.moveaxis(voltages, 3, 0)
    weight_moved = jnp.moveaxis(weights, 1, 0)

    def one_channel(paired):
        voltage, weight_block = paired
        return beam_power(voltage[0], weight_block) + beam_power(voltage[1], weight_block)

    return lax.map(one_channel, (moved, weight_moved))
```

```python
import functools

import jax
import jax.numpy as jnp
from jax import lax
from jax.experimental import pallas as pl
from jax.experimental.pallas import tpu as pltpu
from jax.sharding import Mesh, PartitionSpec as P

BIN = 8
LANES = 128
AXES = ("ta", "gh", "gl")


def beam_kernel(dims, x_ref, w_ref, o_ref, xf, xt, xb):
    halves, locals_, streams, channels, samples, beams, groups = dims
    antennas = locals_ * streams
    bins = samples // BIN
    owned = beams // groups
    stack = LANES // owned
    own_bins = bins // halves
    rows = own_bins // stack
    tile = 256
    block = 256

    def widen(source, carry):
        for chunk in range(0, samples, LANES):
            xf[source, chunk // LANES] = x_ref[source, :, chunk : chunk + LANES].astype(
                jnp.float32
            )
        return carry

    lax.fori_loop(0, halves * locals_, widen, 0)

    def one_channel(channel, carry):
        for half in range(halves):
            for chunk in range(0, samples, LANES):
                parts = []
                for part in range(2):
                    for local in range(locals_):
                        rows_of = pl.ds(part * channels + channel, streams, stride=2 * channels)
                        parts.append(xf[half * locals_ + local, chunk // LANES, rows_of, :])
                xt[half, chunk : chunk + LANES, :] = jnp.concatenate(parts, axis=0).T
        for half in range(halves):
            for index in range(BIN):
                base = (half * BIN + index) * bins
                xb[base : base + bins, :] = xt[half, pl.ds(index, bins, stride=BIN), :].astype(
                    jnp.bfloat16
                )
        w_re = w_ref[channel, 0]
        w_im = w_ref[channel, 1]
        for column in range(0, beams, tile):
            a = w_re[:, column : column + tile]
            b = w_im[:, column : column + tile]
            for_re = jnp.concatenate([a, -b], axis=0)
            for_im = jnp.concatenate([b, a], axis=0)
            total = jnp.zeros((bins, tile), jnp.float32)
            for base in range(0, halves * samples, block):
                lhs = xb[base : base + block, :]
                re = jnp.dot(lhs, for_re, preferred_element_type=jnp.float32)
                im = jnp.dot(lhs, for_im, preferred_element_type=jnp.float32)
                power = re * re + im * im
                for piece in range(0, block, bins):
                    total = total + power[piece : piece + bins]
            lane = lax.broadcasted_iota(jnp.int32, (rows, LANES), 1) // owned
            for group in range(0, tile, LANES):
                for half in range(halves):
                    parts = [
                        total[
                            half * own_bins + k * rows : half * own_bins + (k + 1) * rows,
                            group : group + LANES,
                        ]
                        for k in range(stack)
                    ]
                    for dest in range(stack):
                        out = None
                        for k in range(stack):
                            turn = ((k - dest) * owned) % LANES
                            moved = parts[k] if turn == 0 else pltpu.roll(parts[k], turn, 1)
                            out = moved if out is None else jnp.where(lane == k, moved, out)
                        number = half * groups + (column + group) // owned + dest
                        o_ref[number, channel] = out
        return carry

    lax.fori_loop(0, channels, one_channel, 0)


def form_beams(x, w, halves, groups):
    sources, streams, _, channels, samples = x.shape
    beams = w.shape[3]
    locals_ = sources // halves
    bins = samples // BIN
    owned = beams // groups
    rows = bins // halves * owned // LANES
    antennas = locals_ * streams
    dims = (halves, locals_, streams, channels, samples, beams, groups)
    flops = 2 * channels * halves * samples * 2 * beams * 2 * antennas
    vmem = pl.BlockSpec(memory_space=pltpu.VMEM)
    return pl.pallas_call(
        functools.partial(beam_kernel, dims),
        out_shape=jax.ShapeDtypeStruct((halves * groups, channels, rows, LANES), jnp.float32),
        in_specs=[vmem, vmem],
        out_specs=vmem,
        scratch_shapes=[
            pltpu.VMEM((sources, samples // LANES, streams * 2 * channels, LANES), jnp.float32),
            pltpu.VMEM((halves, samples, 2 * antennas), jnp.float32),
            pltpu.VMEM((halves * samples, 2 * antennas), jnp.bfloat16),
        ],
        compiler_params=pltpu.CompilerParams(vmem_limit_bytes=40 << 20),
        cost_estimate=pl.CostEstimate(flops=flops, bytes_accessed=4 << 20, transcendentals=0),
        name="form_beams",
    )(x.reshape(sources, streams * 2 * channels, samples), w)


def gather_kernel(dims, own_ref, other_ref, o_ref, turned_ref):
    halves, locals_, channels, rows, owned = dims
    stack = LANES // owned
    for side in range(2):
        for row in range(rows):
            parts = []
            for block in range(2):
                ref = own_ref if block == side else other_ref
                for local in range(locals_):
                    for half in range(halves):
                        source = (half * 2 + side) * locals_ + local
                        parts.append(ref[source, pl.ds(row, channels, stride=rows), :])
            table = jnp.concatenate(parts, axis=0)
            for column in range(0, table.shape[0], LANES):
                turned = table[column : column + LANES].T
                for k in range(stack):
                    places = pl.ds(k * rows + row, owned, stride=stack * rows)
                    turned_ref[column // LANES, places, :] = turned[k * owned : (k + 1) * owned]
        for column in range(turned_ref.shape[0]):
            o_ref[side, :, column * LANES : (column + 1) * LANES] = turned_ref[column]


def gather_spectra(own, other, halves, owned):
    sources, channels, rows, _ = own.shape
    locals_ = sources // (2 * halves)
    dims = (halves, locals_, channels, rows, owned)
    count = 2 * locals_ * halves * channels
    bins = rows * LANES // owned
    vmem = pl.BlockSpec(memory_space=pltpu.VMEM)
    out = pl.pallas_call(
        functools.partial(gather_kernel, dims),
        out_shape=jax.ShapeDtypeStruct((2, owned * bins, count), jnp.float32),
        in_specs=[vmem, vmem],
        out_specs=vmem,
        scratch_shapes=[pltpu.VMEM((count // LANES, owned * bins, LANES), jnp.float32)],
        compiler_params=pltpu.CompilerParams(vmem_limit_bytes=40 << 20),
        name="gather_spectra",
    )(
        own.reshape(sources, channels * rows, LANES),
        other.reshape(sources, channels * rows, LANES),
    )
    return out.reshape(2, owned, bins, count).transpose(3, 0, 1, 2)


def plain_beams(x, w, halves, groups):
    sources, streams, _, channels, samples = x.shape
    beams = w.shape[3]
    antennas = sources // halves * streams
    v = x.reshape(halves, antennas, 2, channels, samples)
    args = dict(preferred_element_type=jnp.float32)
    rr = jnp.einsum("jab,hajs->hjbs", w[:, 0], v[:, :, 0], **args)
    ii = jnp.einsum("jab,hajs->hjbs", w[:, 1], v[:, :, 1], **args)
    ri = jnp.einsum("jab,hajs->hjbs", w[:, 0], v[:, :, 1], **args)
    ir = jnp.einsum("jab,hajs->hjbs", w[:, 1], v[:, :, 0], **args)
    re, im = rr - ii, ri + ir
    power = (re * re + im * im).reshape(halves, channels, beams, samples // BIN, BIN)
    total = power.sum((0, 4)).reshape(channels, groups, beams // groups, halves, -1)
    return total.transpose(3, 1, 0, 2, 4).reshape(
        halves * groups, channels, beams // groups, samples // BIN // halves
    )


def plain_gather(own, other, halves, owned):
    sources, channels, _, bins = own.shape
    locals_ = sources // (2 * halves)
    sides = []
    for side in range(2):
        blocks = []
        for block in range(2):
            part = (own if block == side else other).reshape(
                halves, 2, locals_, channels, owned, bins
            )[:, side]
            blocks.append(part.transpose(1, 0, 2, 3, 4))
        sides.append(jnp.stack(blocks).reshape(-1, owned, bins))
    return jnp.stack(sides, 1)


def on_device(halves, groups, voltages, weights):
    _, streams, _, channel_total, samples = voltages.shape
    locals_ = groups // 2
    part = channel_total // (groups * halves)
    beams = weights.shape[3]
    owned = beams // groups
    tiled = (
        LANES % owned == 0
        and samples // BIN // halves * owned == 8 * LANES
        and streams == 8
        and part == 8
        and beams % 256 == 0
    )
    side = lax.axis_index("gh")
    half = lax.axis_index("ta")

    w = weights.reshape((2, halves, part) + weights.shape[2:])
    w = lax.dynamic_index_in_dim(w, half, 1, keepdims=False).transpose(0, 1, 2, 4, 3)
    w_own = lax.dynamic_index_in_dim(w, side, 0, keepdims=False)
    w_sent = lax.dynamic_index_in_dim(w, 1 - side, 0, keepdims=False)
    w_other = lax.ppermute(w_sent, "gh", [(0, 1), (1, 0)])

    v = voltages.reshape(streams, 2, 2, locals_, halves, part, samples)
    moved = []
    for block in range(2):
        piece = lax.dynamic_index_in_dim(v, side ^ block, 2, keepdims=False)
        piece = piece.transpose(3, 2, 0, 1, 4, 5).reshape(
            halves * locals_, streams, 2, part, samples
        )
        moved.append(lax.all_to_all(piece, ("ta", "gl"), 0, 0, tiled=True))
    form = form_beams if tiled else plain_beams
    gather = gather_spectra if tiled else plain_gather
    spectra = []
    for block in range(2):
        pieces = form(moved[block], w_own if block == 0 else w_other, halves, groups)
        spectra.append(lax.all_to_all(pieces, AXES, 0, 0, tiled=True))
    return gather(spectra[0], spectra[1], halves, owned)


def solution(mesh):
    halves, groups = mesh.shape["ta"], mesh.shape["gx"]
    cut = Mesh(mesh.devices.reshape(halves, 2, groups // 2), AXES)
    in_specs = (
        P("ta", ("gh", "gl"), None, None, None),
        P(None, ("gh", "gl"), None, None, None),
    )
    out_specs = P(None, None, ("gh", "gl"), "ta")
    return jax.shard_map(
        functools.partial(on_device, halves, groups),
        mesh=cut,
        in_specs=in_specs,
        out_specs=out_specs,
        check_vma=False,
    )
```
